32 devices in a mesh: groups: 2 (over y), ep: 8 (over z, core), tp: 2 (over x).
Axes of the slice: x: 2, y: 2, z: 4, core: 2. Of those that a mesh axis runs over, the one named last changes fastest.
Arguments:
- hidden: bfloat16 [1024, 2880], P(('groups', 'ep')), parts along dimension 0, may hold values from -6 to 6
- route_experts: int32 [1024, 4], P(('groups', 'ep')), parts along dimension 0, may hold values from 0 to 7, all different within a row; in each aligned block of 64 rows (0 to 63, 64 to 127, ...) at most 64 rows name the same one
- route_weight: float32 [1024, 4], P(('groups', 'ep')), parts along dimension 0, may hold values from 0.1 to 0.6
- norm_gain: bfloat16 [2880], replicated, may hold values from 0.099609375 to 1.8984375
- gate_up_codes: int32 [8, 360, 5120], P('ep', None, 'tp'), may hold values from -2147483648 to 2147483646
- gate_up_scales: bfloat16 [8, 90, 5120], P('ep', None, 'tp'), as said below
- gate_up_bias: bfloat16 [8, 5120], P('ep', 'tp'), may hold values from -3 to 3
- down_codes: int32 [8, 2560, 360], P('ep', 'tp'), may hold values from -2147483648 to 2147483646
- down_scales: bfloat16 [8, 80, 2880], P('ep', 'tp'), as said below
- down_bias: bfloat16 [8, 2880], P('ep', 'tp'), may hold values from -3 to 3
Outputs:
- layer_out: bfloat16 [1024, 2880], P(('groups', 'ep'), 'tp'), parts along dimension 0
The draws below stay inside these ranges and needn't reach their ends.
There are 2 independent parts, one for each index of `groups`. The reference program is written for one: setup_inputs(seed, part) draws one part's arguments, and reference() takes and returns one part's arrays. A program takes and returns all parts, laid end to end along the dimension named above; an argument that names none is the same for every part. Nothing has to cross between parts.
Inputs may be any that keep to these rules, and one draw needn't show every extreme that they name: `route_experts`: each row names 4 different experts. In each aligned block of 64 rows no expert is named by more than 64 rows, and in some blocks one expert is named by exactly 64 rows. `gate_up_scales`: every scale is a power of two. `down_scales`: every scale is a power of two.
All inputs are finite; a program needn't handle non-finite values.
Results may differ from the reference program's by a relative error of at most 0.013.
Values may be sent and summed in bfloat16 or wider, within the bound.
A program may use at most 128 MiB of HBM per device.

```python
import math
import jax
import jax.numpy as jnp
import numpy as np
from jax import lax

D = 2880
TOP = 4
FF = 2560
TOK_EP = 64
EXPERTS = 8
TOKENS = 512
CAP = 64
N_EP = 8
N_TP = 2


def draw_gate_up_scales(key, part):
    centre = int(math.floor(math.log2(0.5 / math.sqrt(D))))
    powers = jax.random.randint(jax.random.fold_in(key, 11), (EXPERTS, D // 32, 2 * FF), centre - 1, centre + 2)
    return jnp.exp2(powers.astype(jnp.float32)).astype(jnp.bfloat16)


def draw_down_scales(key, part):
    centre = int(math.floor(math.log2(0.5 / math.sqrt(FF))))
    powers = jax.random.randint(jax.random.fold_in(key, 23), (EXPERTS, FF // 32, D), centre - 1, centre + 2)
    return jnp.exp2(powers.astype(jnp.float32)).astype(jnp.bfloat16)


def place_ends(entries, stream_key, smallest, largest):
    extent = entries.shape
    index_at = [jax.random.randint(jax.random.fold_in(stream_key, axis), (), 0, extent[axis]) for axis in range(len(extent))]
    entries = entries.at[tuple(index_at)].set(smallest)
    longest = extent.index(max(extent))
    index_at[longest] = (index_at[longest] + 1) % extent[longest]
    return entries.at[tuple(index_at)].set(largest)


def shard_levels(own_key, extent, cuts, low, high):
    def one(axis_at, blocks):
        heights = jax.random.uniform(jax.random.fold_in(jax.random.fold_in(own_key, 6), axis_at), (blocks,), jnp.float32, low / len(cuts), high / len(cuts))
        return jnp.repeat(jnp.exp(heights), extent[axis_at] // blocks).reshape((-1,) + (1,) * (len(extent) - axis_at - 1))

    level = one(*cuts[0])
    for cut in cuts[1:]:
        level = level * one(*cut)
    return level


def shared_out(rng, own, number, rows, amount, top, reach, slope):
    ranking = jax.random.permutation(rng, amount)
    crowded, common = load_shares(amount, rows * top, reach, slope, True), load_shares(amount, rows * top, reach, slope, False)
    places = jnp.arange(amount)

    def named(lengths, offset_by):
        used = int((lengths > 0).sum())
        fixed = max(1, used // 4)
        moved = fixed + (places - fixed + offset_by * (used - fixed)) % max(1, amount - fixed)
        return jnp.zeros((amount,), jnp.int32).at[ranking[jnp.where(places < fixed, places, moved)]].set(jnp.asarray(lengths, jnp.int32))

    lengths = jnp.where(number % 4 == 0, named(crowded, number // 4), named(common, number - number // 4 - 1))
    mixed = jax.random.permutation(jax.random.fold_in(own, 3), amount)
    giver, taker = mixed[0:amount // 2 * 2:2], mixed[1:amount // 2 * 2:2]
    margin = jnp.minimum(lengths[giver] - 1, reach - lengths[taker]) // 2
    margin = jnp.where((giver == ranking[0]) | (taker == ranking[0]) | (lengths[taker] == 0), 0, jnp.maximum(margin, 0))
    moved = jax.random.randint(jax.random.fold_in(own, 4), (amount // 2,), 0, 1 << 20) % (margin + 1)
    lengths = lengths.at[giver].add(-moved).at[taker].add(moved)
    items = jnp.searchsorted(jnp.cumsum(lengths), jnp.arange(rows * top), side="right").astype(jnp.int32)
    grid = items.reshape(top, rows).T
    grid = grid[jax.random.permutation(jax.random.fold_in(own, 1), rows)]
    offset_by = jax.random.randint(jax.random.fold_in(own, 2), (rows, 1), 0, top)
    return jnp.take_along_axis(grid, (jnp.arange(top)[None, :] + offset_by) % top, axis=1)


def load_shares(number_of, total, reach, skew, full):
    portions = [(1 << 20) // math.isqrt(standing ** skew) + 1 for standing in range(1, number_of + 1)]
    largest = reach if full else min(reach, max(-(-total // number_of), total * portions[0] // sum(portions)))
    least = 1 if total - largest >= number_of - 1 else 0
    holding, surplus = [largest] + [least] * (number_of - 1), total - largest - least * (number_of - 1)
    while surplus > 0:
        free = [i for i in range(1, number_of) if holding[i] < largest] or [i for i in range(1, number_of) if holding[i] < reach]
        whole, budget = sum([portions[i] for i in free]), surplus
        for i in free:
            extra = min(reach - holding[i], max(1, budget * portions[i] // whole), surplus)
            holding[i] = holding[i] + extra
            surplus = surplus - extra
    return np.array(holding)


def bell_draw(rng, extent, spread, reach, shards=(), held_as=jnp.bfloat16):
    gain = shard_levels(rng, extent, shards, -0.22, 0.18) if shards else 1.0
    entries = jax.random.normal(rng, extent, jnp.float32) * spread * gain
    return jnp.minimum(jnp.maximum(entries, -reach), reach).astype(held_as)


def setup_inputs(seed: int = 0, part: int = 0) -> dict:
    key_of = jax.random.split(jax.random.key(seed), 11)
    part_splits = jax.random.split(jax.random.fold_in(key_of[10], part), 11)
    hidden = bell_draw(part_splits[0], (TOKENS, D), 1.0, 6.0, ((0, 8),))
    route_experts_keys = jax.random.split(jax.random.fold_in(part_splits[1], 1), TOKENS // TOK_EP)
    route_experts_turns = jax.random.permutation(jax.random.fold_in(part_splits[1], 3), TOKENS // TOK_EP)
    route_experts = jax.vmap(lambda own, number: shared_out(jax.random.fold_in(part_splits[1], 2), own, number, TOK_EP, EXPERTS, TOP, CAP, 2))(route_experts_keys, route_experts_turns).reshape((TOKENS, TOP))
    route_weight = jnp.clip(0.1 + 0.5 * jax.random.uniform(part_splits[2], (TOKENS, TOP), jnp.float32) ** shard_levels(part_splits[2], (TOKENS, TOP), ((0, 8),), -0.2, 0.2), 0.1, 0.6)
    norm_gain = jnp.clip(1.0 + 0.18 * jax.random.normal(key_of[3], (D,), jnp.float32), 0.099609375, 1.8984375).astype(jnp.bfloat16)
    gate_up_codes = place_ends(jax.random.randint(key_of[4], (EXPERTS, D // 8, 2 * FF), -2147483648, 2147483647), jax.random.fold_in(key_of[4], 1), -2147483648, 2147483646).astype(jnp.int32)
    gate_up_scales = draw_gate_up_scales(jax.random.fold_in(key_of[10], 71), part)
    gate_up_bias = bell_draw(key_of[6], (EXPERTS, 2 * FF), 0.5, 3.0, ((0, 8), (1, 2)))
    down_codes = place_ends(jax.random.randint(key_of[7], (EXPERTS, FF, D // 8), -2147483648, 2147483647), jax.random.fold_in(key_of[7], 1), -2147483648, 2147483646).astype(jnp.int32)
    down_scales = draw_down_scales(jax.random.fold_in(key_of[10], 71), part)
    down_bias = bell_draw(key_of[9], (EXPERTS, D), 0.5, 3.0, ((0, 8), (1, 2)))
    return {"hidden": hidden, "route_experts": route_experts, "route_weight": route_weight, "norm_gain": norm_gain, "gate_up_codes": gate_up_codes, "gate_up_scales": gate_up_scales, "gate_up_bias": gate_up_bias, "down_codes": down_codes, "down_scales": down_scales, "down_bias": down_bias}


def decode_nibble(nibble):
    magnit = nibble & 7
    exponent = jnp.maximum(jnp.right_shift(magnit, 1) - 1, 0)
    doubled = jnp.where(magnit < 2, magnit, jnp.left_shift(2 + (magnit & 1), exponent))
    signed_val = doubled.astype(jnp.float32) * 0.5
    return jnp.where(nibble >= 8, -signed_val, signed_val)

def unpack_weights(packed, scaling):
    row_count = packed.shape[0]
    shifts = jnp.arange(8, dtype=jnp.int32) * 4
    nibble = jnp.right_shift(packed[:, :, None], shifts[None, None, :]) & 15
    nibble = nibble.reshape(row_count, packed.shape[1] * 8)
    signed_val = decode_nibble(nibble)
    signed_val = signed_val.reshape(row_count // 32, 32, -1) * scaling.astype(jnp.float32)[:, None, :]
    return signed_val.reshape(row_count, -1).astype(jnp.bfloat16)

def unpack_rows(packed, scaling):
    row_count = packed.shape[0] * 8
    shifts = jnp.arange(8, dtype=jnp.int32) * 4
    nibble = jnp.right_shift(packed[:, None, :], shifts[None, :, None]) & 15
    nibble = nibble.reshape(row_count, packed.shape[1])
    signed_val = decode_nibble(nibble)
    signed_val = signed_val.reshape(row_count // 32, 32, -1) * scaling.astype(jnp.float32)[:, None, :]
    return signed_val.reshape(row_count, -1).astype(jnp.bfloat16)

def rms_normed(hidden, norm_gain):
    widened = hidden.astype(jnp.float32)
    mean_square = lax.optimization_barrier(jnp.mean(widened * widened, axis=-1, keepdims=True))
    scaled = widened * lax.rsqrt(mean_square + 1e-05) * norm_gain.astype(jnp.float32)
    return scaled.astype(jnp.bfloat16)

def slot_numbers(routes):
    block_count, row_count, top_count = routes.shape
    flat_routes = routes.reshape(block_count, row_count * top_count)
    onehot = (flat_routes[:, :, None] == jnp.arange(EXPERTS, dtype=jnp.int32)[None, None, :]).astype(jnp.int32)
    before = jnp.cumsum(onehot, axis=1) - onehot
    slot_of = lax.optimization_barrier(jnp.sum(before * onehot, axis=2))
    return slot_of.reshape(block_count, row_count, top_count)

def expert_rows(normed_rows, gate_codes, gate_scales, gate_bias, lower_codes, lower_scales, lower_bias):
    gate_up_weight = unpack_rows(gate_codes, gate_scales)
    down_weight = unpack_weights(lower_codes, lower_scales)
    projected = jnp.dot(normed_rows, gate_up_weight, preferred_element_type=jnp.float32) + gate_bias.astype(jnp.float32)
    gate_part = jnp.minimum(projected[:, 0::2], 7.0)
    upward = jnp.clip(projected[:, 1::2], -7.0, 7.0)
    activated = (gate_part * jax.nn.sigmoid(1.702 * gate_part) * (upward + 1.0)).astype(jnp.bfloat16)
    quarter = FF // N_TP
    summed = jnp.zeros((normed_rows.shape[0], D), jnp.float32)
    for tp_part in range(N_TP):
        partial_value = jnp.dot(activated[:, tp_part * quarter:(tp_part + 1) * quarter], down_weight[tp_part * quarter:(tp_part + 1) * quarter], preferred_element_type=jnp.float32).astype(jnp.bfloat16)
        summed = summed + partial_value.astype(jnp.float32)
    return (summed + lower_bias.astype(jnp.float32)).astype(jnp.bfloat16)

def reference(hidden, route_experts, route_weight, norm_gain, gate_up_codes, gate_up_scales, gate_up_bias, down_codes, down_scales, down_bias):
    normed = rms_normed(hidden, norm_gain)
    routes = route_experts.reshape(N_EP, TOK_EP, TOP)
    slot_of = slot_numbers(routes)
    token_ids = jnp.broadcast_to(jnp.arange(TOKENS, dtype=jnp.int32).reshape(N_EP, TOK_EP, 1), routes.shape)
    block_ids = jnp.broadcast_to(jnp.arange(N_EP, dtype=jnp.int32).reshape(N_EP, 1, 1), routes.shape)
    slot_table = jnp.zeros((EXPERTS, N_EP, CAP), jnp.int32).at[routes, block_ids, slot_of].set(token_ids)

    def one_expert(expert):
        picked = normed[slot_table[expert].reshape(-1)]
        return expert_rows(picked, gate_up_codes[expert], gate_up_scales[expert], gate_up_bias[expert], down_codes[expert], down_scales[expert], down_bias[expert])
    outputs = lax.map(one_expert, jnp.arange(EXPERTS, dtype=jnp.int32)).reshape(EXPERTS, N_EP, CAP, D)
    weights = route_weight.reshape(N_EP, TOK_EP, TOP)
    running = hidden.astype(jnp.float32).reshape(N_EP, TOK_EP, D)
    for position in range(TOP):
        fetched = outputs[routes[:, :, position], block_ids[:, :, position], slot_of[:, :, position]]
        running = running + weights[:, :, position][:, :, None] * fetched.astype(jnp.float32)
    return running.reshape(TOKENS, D).astype(jnp.bfloat16)
```

```python
import functools

import jax
import jax.numpy as jnp
from jax import lax
from jax.experimental import pallas as pl
from jax.experimental.pallas import tpu as pltpu
from jax.sharding import PartitionSpec as P

MAGNITUDES = 0xC8643210 - (1 << 32)
SPARE = 64


def decode_nibble(nibble):
    magnit = nibble & 7
    exponent = jnp.maximum(jnp.right_shift(magnit, 1) - 1, 0)
    doubled = jnp.where(magnit < 2, magnit, jnp.left_shift(2 + (magnit & 1), exponent))
    signed_val = doubled.astype(jnp.float32) * 0.5
    return jnp.where(nibble >= 8, -signed_val, signed_val)


def unpack_weights(packed, scaling):
    row_count = packed.shape[0]
    shifts = jnp.arange(8, dtype=jnp.int32) * 4
    nibble = jnp.right_shift(packed[:, :, None], shifts[None, None, :]) & 15
    nibble = nibble.reshape(row_count, packed.shape[1] * 8)
    signed_val = decode_nibble(nibble)
    signed_val = (
        signed_val.reshape(row_count // 32, 32, -1) * scaling.astype(jnp.float32)[:, None, :]
    )
    return signed_val.reshape(row_count, -1).astype(jnp.bfloat16)


def unpack_rows(packed, scaling):
    row_count = packed.shape[0] * 8
    shifts = jnp.arange(8, dtype=jnp.int32) * 4
    nibble = jnp.right_shift(packed[:, None, :], shifts[None, :, None]) & 15
    nibble = nibble.reshape(row_count, packed.shape[1])
    signed_val = decode_nibble(nibble)
    signed_val = (
        signed_val.reshape(row_count // 32, 32, -1) * scaling.astype(jnp.float32)[:, None, :]
    )
    return signed_val.reshape(row_count, -1).astype(jnp.bfloat16)


def rms_normed(hidden, norm_gain):
    widened = hidden.astype(jnp.float32)
    mean_square = jnp.mean(widened * widened, axis=-1, keepdims=True)
    scaled = widened * lax.rsqrt(mean_square + 1e-05) * norm_gain.astype(jnp.float32)
    return scaled.astype(jnp.bfloat16)


def shards(
    hidden,
    route_experts,
    route_weight,
    norm_gain,
    gate_up_codes,
    gate_up_scales,
    gate_up_bias,
    down_codes,
    down_scales,
    down_bias,
):
    ep_count = lax.axis_size("ep")
    tp_count = lax.axis_size("tp")
    tp_rank = lax.axis_index("tp")
    tok_count, model_width = hidden.shape
    top_count = route_experts.shape[1]
    capacity = min(tok_count, max(tp_count, 2 * tok_count * top_count // ep_count))
    normed = rms_normed(hidden, norm_gain)
    flat_routes = route_experts.reshape(-1)
    onehot = (flat_routes[:, None] == jnp.arange(ep_count, dtype=jnp.int32)[None, :]).astype(
        jnp.int32
    )
    before = jnp.cumsum(onehot, axis=0) - onehot
    slot_of = jnp.sum(before * onehot, axis=1)
    target = (flat_routes * capacity + slot_of).reshape(tok_count, top_count)
    columns = jnp.arange(ep_count * capacity, dtype=jnp.int32)
    matches = target[:, :, None] == columns[None, None, :]
    placing = jnp.any(matches, axis=1).astype(jnp.bfloat16)
    weighting = jnp.sum(jnp.where(matches, route_weight[:, :, None], 0.0), axis=1)
    outgoing = lax.dot_general(
        placing, normed, (((0,), (0,)), ((), ())), preferred_element_type=jnp.float32
    ).astype(jnp.bfloat16)
    outgoing = outgoing.reshape(ep_count, capacity, model_width)
    gate_up_weight = unpack_rows(gate_up_codes[0], gate_up_scales[0])
    down_weight = unpack_weights(down_codes[0], down_scales[0])
    arrived = lax.all_to_all(outgoing, "ep", split_axis=0, concat_axis=0, tiled=True)
    source_count, item_count, _ = arrived.shape
    flat_rows = arrived.reshape(source_count * item_count, model_width)
    projected = jnp.dot(
        flat_rows, gate_up_weight, preferred_element_type=jnp.float32
    ) + gate_up_bias[0].astype(jnp.float32)
    gate_part = jnp.minimum(projected[:, 0::2], 7.0)
    upward = jnp.clip(projected[:, 1::2], -7.0, 7.0)
    activated = (gate_part * jax.nn.sigmoid(1.702 * gate_part) * (upward + 1.0)).astype(
        jnp.bfloat16
    )
    partial_value = jnp.dot(activated, down_weight, preferred_element_type=jnp.float32)
    partial_value = partial_value.astype(jnp.bfloat16).astype(jnp.float32)
    partial_value = partial_value.reshape(source_count, item_count, model_width)
    summed = lax.psum_scatter(
        partial_value.astype(jnp.bfloat16), "tp", scatter_dimension=2, tiled=True
    ).astype(jnp.float32)
    answered = (summed + down_bias[0].astype(jnp.float32)).astype(jnp.bfloat16)
    came_back = lax.all_to_all(answered, "ep", split_axis=0, concat_axis=0, tiled=True)
    quarter = model_width // tp_count
    own_cols = lax.dynamic_slice_in_dim(hidden, tp_rank * quarter, quarter, 1).astype(jnp.float32)
    gathered = came_back.reshape(ep_count * capacity, quarter).astype(jnp.float32)
    layer_out = own_cols + jnp.dot(weighting, gathered, precision=lax.Precision.HIGHEST)
    return layer_out.astype(jnp.bfloat16)


def xor_peer(z, d):
    if d & 1:
        z = z + 1 - 2 * (z % 2)
    if d & 2:
        z = z + 2 - 4 * ((z // 2) % 2)
    return z


def layer_kernel(
    sizes,
    payload,
    own_cols,
    gate_codes,
    gate_scales,
    gate_bias,
    down_codes,
    down_scales,
    down_bias,
    out,
    rows_in,
    gate_weight,
    down_weight,
    padded_codes,
    activated,
    pair_out,
    pair_in,
    side_out,
    side_in,
    kept,
    far_out,
    far_in,
    own_send,
    own_recv,
    disp_send,
    disp_recv,
    cross_send,
    cross_recv,
    fwd_send,
    fwd_recv,
    pair_send,
    pair_recv,
    side_send,
    side_recv,
    far_send,
    far_recv,
):
    tok, width, n_z = sizes
    half_rows = tok // 2
    half_cols = width // 2
    ep = lax.axis_index("ep")
    x = lax.axis_index("tp")
    z = ep // 2
    core = ep % 2
    partner = {"ep": 2 * z + 1 - core}
    across = {"tp": 1 - x}

    def far(d):
        return {"ep": 2 * xor_peer(z, d) + core}

    def copy(src, dst, send, recv, device):
        return pltpu.make_async_remote_copy(
            src_ref=src,
            dst_ref=dst,
            send_sem=send,
            recv_sem=recv,
            device_id=device,
            device_id_type=pl.DeviceIdType.MESH,
        )

    barrier = pltpu.get_barrier_semaphore()
    for device in [partner, across] + [far(d) for d in range(1, n_z)]:
        pl.semaphore_signal(
            barrier, inc=1, device_id=device, device_id_type=pl.DeviceIdType.MESH
        )
    pl.semaphore_wait(barrier, n_z + 1)

    def block_rows(owner, half=None):
        if half is None:
            return rows_in.at[pl.ds(pl.multiple_of(owner * tok, tok), tok)]
        start = owner * tok + half * half_rows
        return rows_in.at[pl.ds(pl.multiple_of(start, half_rows), half_rows)]

    own_half = payload.at[pl.ds(pl.multiple_of(x * half_rows, half_rows), half_rows)]
    disp = [
        copy(own_half, block_rows(ep, x), disp_send.at[d], disp_recv.at[d], far(d))
        for d in range(1, n_z)
    ]
    own = copy(payload, block_rows(ep), own_send, own_recv, partner)
    for step in disp:
        step.start()
    own.start()
    rows_in[pl.ds(pl.multiple_of(ep * tok, tok), tok), :] = payload[...]

    def arriving(d, half):
        return block_rows(2 * xor_peer(z, d) + core, half)

    crossing = [
        copy(arriving(d, x), arriving(d, x), cross_send.at[d], cross_recv.at[d], across)
        for d in range(1, n_z)
    ]
    passing = [
        [
            copy(arriving(d, h), arriving(d, h), fwd_send.at[d, i], fwd_recv.at[d, i], partner)
            for i, h in enumerate((x, 1 - x))
        ]
        for d in range(1, n_z)
    ]

    def pass_on(d):
        disp[d - 1].wait_recv()
        crossing[d - 1].start()
        passing[d - 1][0].start()

    def pass_crossed(d):
        crossing[d - 1].wait_recv()
        passing[d - 1][1].start()

    place = lax.broadcasted_iota(jnp.int32, (8, 1), 0) * 4
    gate_cols = gate_codes.shape[1]
    col_step = 512 if gate_cols % 512 == 0 else 256

    def gate_rows(s, carry):
        base = pl.multiple_of(s * 8, 8)
        for col in range(0, gate_cols, col_step):
            words = gate_codes[pl.ds(base, 8), col : col + col_step]
            shifted = words
            for group in range(2):
                scale = jnp.broadcast_to(
                    gate_scales[pl.ds(2 * s + group, 1), col : col + col_step], (8, col_step)
                )
                pieces = []
                for w in range(4):
                    row = group * 4 + w
                    one = jnp.broadcast_to(shifted[row : row + 1, :], (8, col_step))
                    place_wide = jnp.broadcast_to(place, (8, col_step))
                    quad = jnp.left_shift(lax.shift_right_logical(one, place_wide), 2) & 28
                    doubled = lax.shift_right_logical(jnp.full_like(one, MAGNITUDES), quad) & 15
                    negative = jnp.left_shift(one, 28 - place_wide) < 0
                    pieces.append(
                        doubled.astype(jnp.float32) * jnp.where(negative, -scale, scale)
                    )
                start = pl.multiple_of(s * 64 + group * 32, 32)
                gate_weight[pl.ds(start, 32), col : col + col_step] = jnp.concatenate(
                    pieces, axis=0
                ).astype(jnp.bfloat16)
        return carry

    gate_steps = gate_codes.shape[0] // 8
    gate_weight[pl.ds(width, SPARE), :] = jnp.zeros((SPARE, gate_cols), jnp.bfloat16)
    cut = gate_steps // 2
    lax.fori_loop(0, cut, gate_rows, 0)
    pass_on(1)
    lax.fori_loop(cut, gate_steps, gate_rows, 0)
    pass_on(2)
    pass_crossed(1)

    code_words = down_codes.shape[1]
    whole_lanes = code_words // 128 * 128
    lane_total = padded_codes.shape[1]
    padded_codes[:, lane_total - 128 :] = jnp.zeros((padded_codes.shape[0], 128), jnp.int32)
    padded_codes[:, 0:whole_lanes] = down_codes[:, 0:whole_lanes]
    padded_codes[:, whole_lanes:code_words] = down_codes[:, whole_lanes:code_words]
    lanes = lax.broadcasted_iota(jnp.int32, (32, 128), 1)
    lane_word = lanes // 8
    lane_place = (lanes % 8) * 4
    lane_sign = 28 - lane_place

    down_steps = down_codes.shape[0] // 32

    def down_rows(h, s, carry):
        base = pl.multiple_of(s * 32, 32)
        sources = [
            padded_codes[pl.ds(base, 32), v * 128 : (v + 1) * 128] for v in range(lane_total // 128)
        ]
        scale_row = down_scales[pl.ds(h * down_steps + s, 1), :]
        for b in range(-(-half_cols // 128)):
            first = h * (half_cols // 8) + 16 * b
            low, high = first // 128, (first + 15) // 128
            index = (lane_word + first % 128) % 128
            words = jnp.take_along_axis(sources[low], index, axis=1, mode="promise_in_bounds")
            if high != low:
                other = jnp.take_along_axis(sources[high], index, axis=1, mode="promise_in_bounds")
                words = jnp.where(lane_word + first % 128 < 128, words, other)
            size = min(128, half_cols - 128 * b)
            scale = jnp.broadcast_to(scale_row[:, 128 * b : 128 * (b + 1)], (32, 128))
            quad = jnp.left_shift(lax.shift_right_logical(words, lane_place), 2) & 28
            doubled = lax.shift_right_logical(jnp.full_like(words, MAGNITUDES), quad) & 15
            negative = jnp.left_shift(words, lane_sign) < 0
            value = (doubled.astype(jnp.float32) * jnp.where(negative, -scale, scale)).astype(
                jnp.bfloat16
            )
            down_weight[h, pl.ds(base, 32), 128 * b : 128 * b + size] = value[:, :size]
        return carry

    lax.fori_loop(0, down_steps, functools.partial(down_rows, 0), 0)
    pass_on(3)
    pass_crossed(2)
    lax.fori_loop(0, down_steps, functools.partial(down_rows, 1), 0)
    pass_crossed(3)
    own.wait_recv()
    for d in range(1, n_z):
        for step in passing[d - 1]:
            step.wait_recv()

    picks = (
        lax.broadcasted_iota(jnp.int32, (256, 128), 0)
        == 2 * lax.broadcasted_iota(jnp.int32, (256, 128), 1)
    ).astype(jnp.float32).astype(jnp.bfloat16)

    def gate_tile(t, carry):
        cols = pl.ds(pl.multiple_of(t * 256, 256), 256)
        projected = jnp.dot(
            rows_in[...], gate_weight[:, cols], preferred_element_type=jnp.float32
        ) + gate_bias[:, cols]
        gate_part = jnp.minimum(projected, 7.0)
        upward = pltpu.roll(jnp.clip(projected, -7.0, 7.0), 255, 1)
        value = gate_part * jax.nn.sigmoid(1.702 * gate_part) * (upward + 1.0)
        activated[:, pl.ds(pl.multiple_of(t * 128, 128), 128)] = jnp.dot(
            value.astype(jnp.bfloat16), picks, preferred_element_type=jnp.float32
        ).astype(jnp.bfloat16)
        return carry

    lax.fori_loop(0, gate_cols // 256, gate_tile, 0)

    tail = lax.broadcasted_iota(jnp.int32, (2 * tok, SPARE), 1)
    pairing = [
        copy(pair_out.at[d], pair_in.at[d], pair_send.at[d], pair_recv.at[d], partner)
        for d in range(n_z)
    ]
    siding = [
        copy(side_out.at[d], side_in.at[d], side_send.at[d], side_recv.at[d], across)
        for d in range(n_z)
    ]
    faring = [
        None if d == 0 else copy(far_out.at[d], far_in.at[d], far_send.at[d], far_recv.at[d], far(d))
        for d in range(n_z)
    ]

    def multiply(d):
        start = pl.multiple_of(xor_peer(z, d) * 2 * tok, 2 * tok)
        rows = activated[pl.ds(start, 2 * tok), :]
        spare = rows_in[pl.ds(start, 2 * tok), width:].astype(jnp.float32)
        hit = (tail == ep) | (tail == ep + 2 * n_z) | (tail == ep + 4 * n_z)
        weight = jnp.sum(jnp.where(hit, spare, 0.0), axis=1, keepdims=True)
        for h in range(2):
            added = down_bias[...] * jnp.where(x == h, 1.0, 0.0)
            value = jnp.dot(rows, down_weight[h], preferred_element_type=jnp.float32) + added
            value = value * weight
            first, second = value[:tok], value[tok:]
            pair_out[d, h] = jnp.where(core == 0, second, first).astype(jnp.bfloat16)
            kept[d, h] = jnp.where(core == 0, first, second).astype(jnp.bfloat16)
        pairing[d].start()

    def fold_pair(d):
        pairing[d].wait_recv()
        sums = [
            kept[d, h].astype(jnp.float32) + pair_in[d, h].astype(jnp.float32) for h in range(2)
        ]
        side_out[d] = jnp.where(x == 0, sums[1], sums[0]).astype(jnp.bfloat16)
        kept[d, 0] = jnp.where(x == 0, sums[0], sums[1]).astype(jnp.bfloat16)
        siding[d].start()

    def fold_side(d):
        siding[d].wait_recv()
        total = kept[d, 0].astype(jnp.float32) + side_in[d].astype(jnp.float32)
        if d == 0:
            return total
        far_out[d] = total.astype(jnp.bfloat16)
        faring[d].start()
        return None

    multiply(3)
    multiply(2)
    fold_pair(3)
    multiply(1)
    fold_pair(2)
    multiply(0)
    fold_pair(1)
    fold_side(3)
    fold_pair(0)
    fold_side(2)
    fold_side(1)
    total = fold_side(0) + own_cols[...].astype(jnp.float32)
    for d in (3, 2, 1):
        faring[d].wait_recv()
        total = total + far_in[d].astype(jnp.float32)
    out[...] = total.astype(jnp.bfloat16)

    own.wait_send()
    for d in range(1, n_z):
        disp[d - 1].wait_send()
        crossing[d - 1].wait_send()
        for step in passing[d - 1]:
            step.wait_send()
        faring[d].wait_send()
    for d in range(n_z):
        pairing[d].wait_send()
        siding[d].wait_send()


def dense_shards(
    hidden,
    route_experts,
    route_weight,
    norm_gain,
    gate_up_codes,
    gate_up_scales,
    gate_up_bias,
    down_codes,
    down_scales,
    down_bias,
):
    ep_count = lax.axis_size("ep")
    tp_rank = lax.axis_index("tp")
    tok, width = hidden.shape
    n_z = ep_count // 2
    half = width // 2
    normed = rms_normed(hidden, norm_gain)
    experts = jnp.arange(ep_count, dtype=jnp.int32)
    per_expert = jnp.sum(
        jnp.where(
            route_experts[:, :, None] == experts[None, None, :], route_weight[:, :, None], 0.0
        ),
        axis=1,
    )
    high = lax.reduce_precision(per_expert, 8, 7)
    middle = lax.reduce_precision(per_expert - high, 8, 7)
    low = per_expert - high - middle
    spare = jnp.concatenate(
        [high, middle, low, jnp.zeros((tok, SPARE - 3 * ep_count), jnp.float32)], axis=1
    ).astype(jnp.bfloat16)
    payload = jnp.concatenate([normed, spare], axis=1)
    own_cols = lax.dynamic_slice_in_dim(hidden, tp_rank * half, half, 1)
    gate_scales = gate_up_scales[0].astype(jnp.float32) * 0.5
    units = down_codes.shape[1]
    lanes = -(-half // 128) * 128
    halves = (down_scales[0].astype(jnp.float32) * 0.5).reshape(-1, 2, half).transpose(1, 0, 2)
    halves = jnp.pad(halves, ((0, 0), (0, 0), (0, lanes - half))).reshape(-1, lanes)
    code_lanes = -(-down_codes.shape[2] // 128) * 128
    bf16 = jnp.bfloat16
    dma = pltpu.SemaphoreType.DMA
    vmem = pltpu.VMEM
    return pl.pallas_call(
        functools.partial(layer_kernel, (tok, width, n_z)),
        out_shape=jax.ShapeDtypeStruct((tok, half), bf16),
        in_specs=[pl.BlockSpec(memory_space=vmem)] * 8,
        out_specs=pl.BlockSpec(memory_space=vmem),
        scratch_shapes=[
            vmem((ep_count * tok, width + SPARE), bf16),
            vmem((width + SPARE, gate_up_codes.shape[2]), bf16),
            vmem((2, units, half), bf16),
            vmem((units, code_lanes), jnp.int32),
            vmem((ep_count * tok, units), bf16),
            vmem((n_z, 2, tok, half), bf16),
            vmem((n_z, 2, tok, half), bf16),
            vmem((n_z, tok, half), bf16),
            vmem((n_z, tok, half), bf16),
            vmem((n_z, 2, tok, half), bf16),
            vmem((n_z, tok, half), bf16),
            vmem((n_z, tok, half), bf16),
            dma,
            dma,
            dma((n_z,)),
            dma((n_z,)),
            dma((n_z,)),
            dma((n_z,)),
            dma((n_z, 2)),
            dma((n_z, 2)),
            dma((n_z,)),
            dma((n_z,)),
            dma((n_z,)),
            dma((n_z,)),
            dma((n_z,)),
            dma((n_z,)),
        ],
        compiler_params=pltpu.CompilerParams(
            collective_id=0, has_side_effects=True, vmem_limit_bytes=63 * 1024 * 1024
        ),
    )(
        payload,
        own_cols,
        gate_up_codes[0],
        gate_scales,
        gate_up_bias.astype(jnp.float32),
        down_codes[0],
        halves,
        down_bias.astype(jnp.float32),
    )


def solution(mesh):
    def layer(*arrays):
        tok, top = arrays[1].shape
        ep_count, tp_count = lax.axis_size("ep"), lax.axis_size("tp")
        dense = 2 * top >= ep_count and tp_count == 2 and ep_count == 8
        return (dense_shards if dense else shards)(*arrays)

    placed = (
        P(("groups", "ep"), None),
        P(("groups", "ep"), None),
        P(("groups", "ep"), None),
        P(),
        P("ep", None, "tp"),
        P("ep", None, "tp"),
        P("ep", "tp"),
        P("ep", "tp", None),
        P("ep", "tp", None),
        P("ep", "tp"),
    )
    return jax.shard_map(
        layer, mesh=mesh, in_specs=placed, out_specs=P(("groups", "ep"), "tp"), check_vma=False
    )
```

```python
import functools

import jax
import jax.numpy as jnp
from jax import lax
from jax.experimental import pallas as pl
from jax.experimental.pallas import tpu as pltpu
from jax.sharding import PartitionSpec as P

MAGNITUDES = 0xC8643210 - (1 << 32)
SPARE = 64


def decode_nibble(nibble):
    magnit = nibble & 7
    exponent = jnp.maximum(jnp.right_shift(magnit, 1) - 1, 0)
    doubled = jnp.where(magnit < 2, magnit, jnp.left_shift(2 + (magnit & 1), exponent))
    signed_val = doubled.astype(jnp.float32) * 0.5
    return jnp.where(nibble >= 8, -signed_val, signed_val)


def unpack_weights(packed, scaling):
    row_count = packed.shape[0]
    shifts = jnp.arange(8, dtype=jnp.int32) * 4
    nibble = jnp.right_shift(packed[:, :, None], shifts[None, None, :]) & 15
    nibble = nibble.reshape(row_count, packed.shape[1] * 8)
    signed_val = decode_nibble(nibble)
    signed_val = (
        signed_val.reshape(row_count // 32, 32, -1) * scaling.astype(jnp.float32)[:, None, :]
    )
    return signed_val.reshape(row_count, -1).astype(jnp.bfloat16)


def unpack_rows(packed, scaling):
    row_count = packed.shape[0] * 8
    shifts = jnp.arange(8, dtype=jnp.int32) * 4
    nibble = jnp.right_shift(packed[:, None, :], shifts[None, :, None]) & 15
    nibble = nibble.reshape(row_count, packed.shape[1])
    signed_val = decode_nibble(nibble)
    signed_val = (
        signed_val.reshape(row_count // 32, 32, -1) * scaling.astype(jnp.float32)[:, None, :]
    )
    return signed_val.reshape(row_count, -1).astype(jnp.bfloat16)


def rms_normed(hidden, norm_gain):
    widened = hidden.astype(jnp.float32)
    mean_square = jnp.mean(widened * widened, axis=-1, keepdims=True)
    scaled = widened * lax.rsqrt(mean_square + 1e-05) * norm_gain.astype(jnp.float32)
    return scaled.astype(jnp.bfloat16)


def shards(
    hidden,
    route_experts,
    route_weight,
    norm_gain,
    gate_up_codes,
    gate_up_scales,
    gate_up_bias,
    down_codes,
    down_scales,
    down_bias,
):
    ep_count = lax.axis_size("ep")
    tp_count = lax.axis_size("tp")
    tp_rank = lax.axis_index("tp")
    tok_count, model_width = hidden.shape
    top_count = route_experts.shape[1]
    capacity = min(tok_count, max(tp_count, 2 * tok_count * top_count // ep_count))
    normed = rms_normed(hidden, norm_gain)
    flat_routes = route_experts.reshape(-1)
    onehot = (flat_routes[:, None] == jnp.arange(ep_count, dtype=jnp.int32)[None, :]).astype(
        jnp.int32
    )
    before = jnp.cumsum(onehot, axis=0) - onehot
    slot_of = jnp.sum(before * onehot, axis=1)
    target = (flat_routes * capacity + slot_of).reshape(tok_count, top_count)
    columns = jnp.arange(ep_count * capacity, dtype=jnp.int32)
    matches = target[:, :, None] == columns[None, None, :]
    placing = jnp.any(matches, axis=1).astype(jnp.bfloat16)
    weighting = jnp.sum(jnp.where(matches, route_weight[:, :, None], 0.0), axis=1)
    outgoing = lax.dot_general(
        placing, normed, (((0,), (0,)), ((), ())), preferred_element_type=jnp.float32
    ).astype(jnp.bfloat16)
    outgoing = outgoing.reshape(ep_count, capacity, model_width)
    gate_up_weight = unpack_rows(gate_up_codes[0], gate_up_scales[0])
    down_weight = unpack_weights(down_codes[0], down_scales[0])
    arrived = lax.all_to_all(outgoing, "ep", split_axis=0, concat_axis=0, tiled=True)
    source_count, item_count, _ = arrived.shape
    flat_rows = arrived.reshape(source_count * item_count, model_width)
    projected = jnp.dot(
        flat_rows, gate_up_weight, preferred_element_type=jnp.float32
    ) + gate_up_bias[0].astype(jnp.float32)
    gate_part = jnp.minimum(projected[:, 0::2], 7.0)
    upward = jnp.clip(projected[:, 1::2], -7.0, 7.0)
    activated = (gate_part * jax.nn.sigmoid(1.702 * gate_part) * (upward + 1.0)).astype(
        jnp.bfloat16
    )
    partial_value = jnp.dot(activated, down_weight, preferred_element_type=jnp.float32)
    partial_value = partial_value.astype(jnp.bfloat16).astype(jnp.float32)
    partial_value = partial_value.reshape(source_count, item_count, model_width)
    summed = lax.psum_scatter(
        partial_value.astype(jnp.bfloat16), "tp", scatter_dimension=2, tiled=True
    ).astype(jnp.float32)
    answered = (summed + down_bias[0].astype(jnp.float32)).astype(jnp.bfloat16)
    came_back = lax.all_to_all(answered, "ep", split_axis=0, concat_axis=0, tiled=True)
    quarter = model_width // tp_count
    own_cols = lax.dynamic_slice_in_dim(hidden, tp_rank * quarter, quarter, 1).astype(jnp.float32)
    gathered = came_back.reshape(ep_count * capacity, quarter).astype(jnp.float32)
    layer_out = own_cols + jnp.dot(weighting, gathered, precision=lax.Precision.HIGHEST)
    return layer_out.astype(jnp.bfloat16)


def xor_peer(z, d):
    if d & 1:
        z = z + 1 - 2 * (z % 2)
    if d & 2:
        z = z + 2 - 4 * ((z // 2) % 2)
    return z


def layer_kernel(
    sizes,
    hidden,
    routes,
    route_weights,
    gain,
    gate_codes,
    gate_scales_in,
    gate_bias,
    down_codes,
    down_scales_in,
    down_bias,
    out,
    payload,
    gate_scales,
    down_scales,
    rows_in,
    gate_weight,
    down_weight,
    padded_codes,
    activated,
    pair_out,
    pair_in,
    side_out,
    side_in,
    kept,
    far_out,
    far_in,
    own_send,
    own_recv,
    disp_send,
    disp_recv,
    cross_send,
    cross_recv,
    fwd_send,
    fwd_recv,
    pair_send,
    pair_recv,
    side_send,
    side_recv,
    far_send,
    far_recv,
):
    tok, width, n_z = sizes
    half_rows = tok // 2
    half_cols = width // 2
    ep = lax.axis_index("ep")
    x = lax.axis_index("tp")
    z = ep // 2
    core = ep % 2
    partner = {"ep": 2 * z + 1 - core}
    across = {"tp": 1 - x}

    def far(d):
        return {"ep": 2 * xor_peer(z, d) + core}

    def copy(src, dst, send, recv, device):
        return pltpu.make_async_remote_copy(
            src_ref=src,
            dst_ref=dst,
            send_sem=send,
            recv_sem=recv,
            device_id=device,
            device_id_type=pl.DeviceIdType.MESH,
        )

    widened = hidden[...].astype(jnp.float32)
    mean_square = jnp.mean(widened * widened, axis=-1, keepdims=True)
    normed = (widened * lax.rsqrt(mean_square + 1e-05) * gain[...].astype(jnp.float32)).astype(
        jnp.bfloat16
    )
    lane = lax.broadcasted_iota(jnp.int32, (tok, SPARE), 1)
    weight_at = jnp.zeros((tok, SPARE), jnp.float32)
    for k in range(routes.shape[1]):
        chosen = routes[:, k : k + 1] == lane % (2 * n_z)
        weight_at = weight_at + jnp.where(chosen, route_weights[:, k : k + 1], 0.0)
    high = weight_at.astype(jnp.bfloat16).astype(jnp.float32)
    middle = (weight_at - high).astype(jnp.bfloat16).astype(jnp.float32)
    low = weight_at - high - middle
    piece = lane // (2 * n_z)
    spare_lanes = jnp.where(
        piece == 0, high, jnp.where(piece == 1, middle, jnp.where(piece == 2, low, 0.0))
    )
    aligned = width // 128 * 128
    payload[:, :aligned] = normed[:, :aligned]
    payload[:, aligned:] = jnp.concatenate(
        [normed[:, aligned:], spare_lanes.astype(jnp.bfloat16)], axis=1
    )

    barrier = pltpu.get_barrier_semaphore()
    for device in [partner, across] + [far(d) for d in range(1, n_z)]:
        pl.semaphore_signal(
            barrier, inc=1, device_id=device, device_id_type=pl.DeviceIdType.MESH
        )
    pl.semaphore_wait(barrier, n_z + 1)

    def block_rows(owner, half=None):
        if half is None:
            return rows_in.at[pl.ds(pl.multiple_of(owner * tok, tok), tok)]
        start = owner * tok + half * half_rows
        return rows_in.at[pl.ds(pl.multiple_of(start, half_rows), half_rows)]

    own_half = payload.at[pl.ds(pl.multiple_of(x * half_rows, half_rows), half_rows)]
    disp = [
        copy(own_half, block_rows(ep, x), disp_send.at[d], disp_recv.at[d], far(d))
        for d in range(1, n_z)
    ]
    own = copy(payload, block_rows(ep), own_send, own_recv, partner)
    for step in disp:
        step.start()
    own.start()
    rows_in[pl.ds(pl.multiple_of(ep * tok, tok), tok), :] = payload[...]

    def arriving(d, half):
        return block_rows(2 * xor_peer(z, d) + core, half)

    crossing = [
        copy(arriving(d, x), arriving(d, x), cross_send.at[d], cross_recv.at[d], across)
        for d in range(1, n_z)
    ]
    passing = [
        [
            copy(arriving(d, h), arriving(d, h), fwd_send.at[d, i], fwd_recv.at[d, i], partner)
            for i, h in enumerate((x, 1 - x))
        ]
        for d in range(1, n_z)
    ]

    def pass_on(d):
        disp[d - 1].wait_recv()
        crossing[d - 1].start()
        passing[d - 1][0].start()

    def pass_crossed(d):
        crossing[d - 1].wait_recv()
        passing[d - 1][1].start()

    gate_scales[...] = gate_scales_in[...].astype(jnp.float32) * 0.5
    scale_rows, scale_lanes = down_scales_in.shape[0], down_scales.shape[1]
    down_scales[:, scale_lanes - 128 :] = jnp.zeros((2 * scale_rows, 128), jnp.float32)
    for h in range(2):
        down_scales[h * scale_rows : (h + 1) * scale_rows, :half_cols] = (
            down_scales_in[:, h * half_cols : (h + 1) * half_cols].astype(jnp.float32) * 0.5
        )
    place = lax.broadcasted_iota(jnp.int32, (8, 1), 0) * 4
    gate_cols = gate_codes.shape[1]
    col_step = 512 if gate_cols % 512 == 0 else 256

    def gate_rows(s, carry):
        base = pl.multiple_of(s * 8, 8)
        for col in range(0, gate_cols, col_step):
            words = gate_codes[pl.ds(base, 8), col : col + col_step]
            shifted = words
            for group in range(2):
                scale = jnp.broadcast_to(
                    gate_scales[pl.ds(2 * s + group, 1), col : col + col_step], (8, col_step)
                )
                pieces = []
                for w in range(4):
                    row = group * 4 + w
                    one = jnp.broadcast_to(shifted[row : row + 1, :], (8, col_step))
                    place_wide = jnp.broadcast_to(place, (8, col_step))
                    quad = jnp.left_shift(lax.shift_right_logical(one, place_wide), 2) & 28
                    doubled = lax.shift_right_logical(jnp.full_like(one, MAGNITUDES), quad) & 15
                    negative = jnp.left_shift(one, 28 - place_wide) < 0
                    pieces.append(
                        doubled.astype(jnp.float32) * jnp.where(negative, -scale, scale)
                    )
                start = pl.multiple_of(s * 64 + group * 32, 32)
                gate_weight[pl.ds(start, 32), col : col + col_step] = jnp.concatenate(
                    pieces, axis=0
                ).astype(jnp.bfloat16)
        return carry

    gate_steps = gate_codes.shape[0] // 8
    gate_weight[pl.ds(width, SPARE), :] = jnp.zeros((SPARE, gate_cols), jnp.bfloat16)
    cut = gate_steps // 2
    lax.fori_loop(0, cut, gate_rows, 0)
    pass_on(1)
    lax.fori_loop(cut, gate_steps, gate_rows, 0)
    pass_on(2)
    pass_crossed(1)

    code_words = down_codes.shape[1]
    whole_lanes = code_words // 128 * 128
    lane_total = padded_codes.shape[1]
    padded_codes[:, lane_total - 128 :] = jnp.zeros((padded_codes.shape[0], 128), jnp.int32)
    padded_codes[:, 0:whole_lanes] = down_codes[:, 0:whole_lanes]
    padded_codes[:, whole_lanes:code_words] = down_codes[:, whole_lanes:code_words]
    lanes = lax.broadcasted_iota(jnp.int32, (32, 128), 1)
    lane_word = lanes // 8
    lane_place = (lanes % 8) * 4
    lane_sign = 28 - lane_place

    down_steps = down_codes.shape[0] // 32

    def down_rows(h, s, carry):
        base = pl.multiple_of(s * 32, 32)
        sources = [
            padded_codes[pl.ds(base, 32), v * 128 : (v + 1) * 128] for v in range(lane_total // 128)
        ]
        scale_row = down_scales[pl.ds(h * down_steps + s, 1), :]
        for b in range(-(-half_cols // 128)):
            first = h * (half_cols // 8) + 16 * b
            low, high = first // 128, (first + 15) // 128
            index = (lane_word + first % 128) % 128
            words = jnp.take_along_axis(sources[low], index, axis=1, mode="promise_in_bounds")
            if high != low:
                other = jnp.take_along_axis(sources[high], index, axis=1, mode="promise_in_bounds")
                words = jnp.where(lane_word + first % 128 < 128, words, other)
            size = min(128, half_cols - 128 * b)
            scale = jnp.broadcast_to(scale_row[:, 128 * b : 128 * (b + 1)], (32, 128))
            quad = jnp.left_shift(lax.shift_right_logical(words, lane_place), 2) & 28
            doubled = lax.shift_right_logical(jnp.full_like(words, MAGNITUDES), quad) & 15
            negative = jnp.left_shift(words, lane_sign) < 0
            value = (doubled.astype(jnp.float32) * jnp.where(negative, -scale, scale)).astype(
                jnp.bfloat16
            )
            down_weight[h, pl.ds(base, 32), 128 * b : 128 * b + size] = value[:, :size]
        return carry

    lax.fori_loop(0, down_steps, functools.partial(down_rows, 0), 0)
    pass_on(3)
    pass_crossed(2)
    lax.fori_loop(0, down_steps, functools.partial(down_rows, 1), 0)
    pass_crossed(3)

    picks = (
        lax.broadcasted_iota(jnp.int32, (256, 128), 0)
        == 2 * lax.broadcasted_iota(jnp.int32, (256, 128), 1)
    ).astype(jnp.float32).astype(jnp.bfloat16)

    def gate_tile(t, carry):
        cols = pl.ds(pl.multiple_of(t * 256, 256), 256)
        projected = jnp.dot(
            rows_in[...], gate_weight[:, cols], preferred_element_type=jnp.float32
        ) + gate_bias[:, cols].astype(jnp.float32)
        gate_part = jnp.minimum(projected, 7.0)
        upward = pltpu.roll(jnp.clip(projected, -7.0, 7.0), 255, 1)
        value = gate_part * jax.nn.sigmoid(1.702 * gate_part) * (upward + 1.0)
        activated[:, pl.ds(pl.multiple_of(t * 128, 128), 128)] = jnp.dot(
            value.astype(jnp.bfloat16), picks, preferred_element_type=jnp.float32
        ).astype(jnp.bfloat16)
        return carry


    tail = lax.broadcasted_iota(jnp.int32, (2 * tok, SPARE), 1)
    pairing = [
        copy(pair_out.at[d], pair_in.at[d], pair_send.at[d], pair_recv.at[d], partner)
        for d in range(n_z)
    ]
    siding = [
        copy(side_out.at[d], side_in.at[d], side_send.at[d], side_recv.at[d], across)
        for d in range(n_z)
    ]
    faring = [
        None if d == 0 else copy(far_out.at[d], far_in.at[d], far_send.at[d], far_recv.at[d], far(d))
        for d in range(n_z)
    ]

    def multiply(d):
        start = pl.multiple_of(xor_peer(z, d) * 2 * tok, 2 * tok)
        rows = activated[pl.ds(start, 2 * tok), :]
        spare = rows_in[pl.ds(start, 2 * tok), width:].astype(jnp.float32)
        hit = (tail == ep) | (tail == ep + 2 * n_z) | (tail == ep + 4 * n_z)
        weight = jnp.sum(jnp.where(hit, spare, 0.0), axis=1, keepdims=True)
        for h in range(2):
            added = down_bias[...].astype(jnp.float32) * jnp.where(x == h, 1.0, 0.0)
            value = jnp.dot(rows, down_weight[h], preferred_element_type=jnp.float32) + added
            value = value * weight
            first, second = value[:tok], value[tok:]
            pair_out[d, h] = jnp.where(core == 0, second, first).astype(jnp.bfloat16)
            kept[d, h] = jnp.where(core == 0, first, second).astype(jnp.bfloat16)
        pairing[d].start()

    def fold_pair(d):
        pairing[d].wait_recv()
        sums = [
            kept[d, h].astype(jnp.float32) + pair_in[d, h].astype(jnp.float32) for h in range(2)
        ]
        side_out[d] = jnp.where(x == 0, sums[1], sums[0]).astype(jnp.bfloat16)
        kept[d, 0] = jnp.where(x == 0, sums[0], sums[1]).astype(jnp.bfloat16)
        siding[d].start()

    def fold_side(d):
        siding[d].wait_recv()
        total = kept[d, 0].astype(jnp.float32) + side_in[d].astype(jnp.float32)
        if d == 0:
            return total
        far_out[d] = total.astype(jnp.bfloat16)
        faring[d].start()
        return None

    def gathered(d):
        for step in passing[d - 1]:
            step.wait_recv()

    own.wait_recv()
    for d in range(1, n_z):
        gathered(d)
    lax.fori_loop(0, gate_cols // 256, gate_tile, 0)
    multiply(3)
    multiply(2)
    fold_pair(3)
    multiply(1)
    fold_pair(2)
    fold_side(3)
    multiply(0)
    fold_pair(1)
    fold_side(2)
    fold_pair(0)
    fold_side(1)
    own_cols = jnp.where(x == 0, hidden[:, :half_cols], hidden[:, half_cols:])
    total = fold_side(0) + own_cols.astype(jnp.float32)
    for d in (1, 3, 2):
        faring[d].wait_recv()
        total = total + far_in[d].astype(jnp.float32)
    out[...] = total.astype(jnp.bfloat16)

    own.wait_send()
    for d in range(1, n_z):
        disp[d - 1].wait_send()
        crossing[d - 1].wait_send()
        for step in passing[d - 1]:
            step.wait_send()
        faring[d].wait_send()
    for d in range(n_z):
        pairing[d].wait_send()
        siding[d].wait_send()


def dense_shards(
    hidden,
    route_experts,
    route_weight,
    norm_gain,
    gate_up_codes,
    gate_up_scales,
    gate_up_bias,
    down_codes,
    down_scales,
    down_bias,
):
    ep_count = lax.axis_size("ep")
    tok, width = hidden.shape
    n_z = ep_count // 2
    half = width // 2
    units = down_codes.shape[1]
    lanes = -(-half // 128) * 128
    code_lanes = -(-down_codes.shape[2] // 128) * 128
    bf16 = jnp.bfloat16
    dma = pltpu.SemaphoreType.DMA
    vmem = pltpu.VMEM
    return pl.pallas_call(
        functools.partial(layer_kernel, (tok, width, n_z)),
        out_shape=jax.ShapeDtypeStruct((tok, half), bf16),
        in_specs=[pl.BlockSpec(memory_space=vmem)] * 10,
        out_specs=pl.BlockSpec(memory_space=vmem),
        scratch_shapes=[
            vmem((tok, width + SPARE), bf16),
            vmem(gate_up_scales.shape[1:], jnp.float32),
            vmem((2 * down_scales.shape[1], lanes), jnp.float32),
            vmem((ep_count * tok, width + SPARE), bf16),
            vmem((width + SPARE, gate_up_codes.shape[2]), bf16),
            vmem((2, units, half), bf16),
            vmem((units, code_lanes), jnp.int32),
            vmem((ep_count * tok, units), bf16),
            vmem((n_z, 2, tok, half), bf16),
            vmem((n_z, 2, tok, half), bf16),
            vmem((n_z, tok, half), bf16),
            vmem((n_z, tok, half), bf16),
            vmem((n_z, 2, tok, half), bf16),
            vmem((n_z, tok, half), bf16),
            vmem((n_z, tok, half), bf16),
            dma,
            dma,
            dma((n_z,)),
            dma((n_z,)),
            dma((n_z,)),
            dma((n_z,)),
            dma((n_z, 2)),
            dma((n_z, 2)),
            dma((n_z,)),
            dma((n_z,)),
            dma((n_z,)),
            dma((n_z,)),
            dma((n_z,)),
            dma((n_z,)),
        ],
        compiler_params=pltpu.CompilerParams(
            collective_id=0, has_side_effects=True, vmem_limit_bytes=63 * 1024 * 1024
        ),
    )(
        hidden,
        route_experts,
        route_weight,
        norm_gain.reshape(1, width),
        gate_up_codes[0],
        gate_up_scales[0],
        gate_up_bias,
        down_codes[0],
        down_scales[0],
        down_bias,
    )


def solution(mesh):
    def layer(*arrays):
        tok, top = arrays[1].shape
        ep_count, tp_count = lax.axis_size("ep"), lax.axis_size("tp")
        dense = 2 * top >= ep_count and tp_count == 2 and ep_count == 8
        return (dense_shards if dense else shards)(*arrays)

    placed = (
        P(("groups", "ep"), None),
        P(("groups", "ep"), None),
        P(("groups", "ep"), None),
        P(),
        P("ep", None, "tp"),
        P("ep", None, "tp"),
        P("ep", "tp"),
        P("ep", "tp", None),
        P("ep", "tp", None),
        P("ep", "tp"),
    )
    return jax.shard_map(
        layer, mesh=mesh, in_specs=placed, out_specs=P(("groups", "ep"), "tp"), check_vma=False
    )
```
